32 devices in a mesh: dp: 8 (over z, x), fsdp: 4 (over y, core).
Axes of the slice: x: 2, y: 2, z: 4, core: 2. Of those that a mesh axis runs over, the one named last changes fastest.
Arguments:
- queries: bfloat16 [8192, 768], P(('dp', 'fsdp')), may hold values from -6 to 6
- keys_values: bfloat16 [8192, 256], P(('dp', 'fsdp')), may hold values from -6 to 6
- seg_ids: int32 [8192], P(('dp', 'fsdp')), may hold values from 0 to 8191, as said below
- in_resp: int32 [8192], P(('dp', 'fsdp')), may hold values from 0 to 1, as said below
- advantage: int32 [8192], P(('dp', 'fsdp')), may hold values from -24 to 24
- out_weight: bfloat16 [768, 1536], P(None, 'fsdp'), may hold values from -0.21875 to 0.21875
- upstream: bfloat16 [8192, 1536], P(('dp', 'fsdp')), may hold values from -6 to 6
Outputs:
- branch_out: bfloat16 [8192, 1536], P(('dp', 'fsdp'))
- grad_queries: bfloat16 [8192, 768], P(('dp', 'fsdp'))
- grad_keys_values: bfloat16 [8192, 256], P(('dp', 'fsdp'))
- grad_weight: float32 [768, 1536], P('dp', 'fsdp')
The draws below stay inside these ranges and needn't reach their ends.
Inputs may be any that keep to these rules, and one draw needn't show every extreme that they name: `seg_ids`: never falling; a token's id is the position of the first token of its sequence; a new sequence begins at the first of every 256 tokens, so no sequence spans two devices. `in_resp`: the last of every 256 tokens is 1.
All inputs are finite; a program needn't handle non-finite values.
Results may differ from the reference program's by a relative error of at most 0.012.
Values may be sent and summed in bfloat16 or wider, within the bound.
A program may use at most 64 MiB of HBM per device.

```python
import jax
import jax.numpy as jnp
from jax import lax

D = 1536
HEADS = 6
HEAD = 128
TOK_DEV = 256
TOKENS = 8192


def draw_seg_ids(key, part):
    place = jnp.arange(TOKENS, dtype=jnp.int32)
    starts = jax.random.randint(key, (TOKENS,), 0, max(TOK_DEV // 4, 2)) == 0
    starts = starts | (place % TOK_DEV == 0) | (place == TOKENS - 1)
    first = jnp.where(starts, place, jnp.zeros_like(place)).astype(jnp.int32)
    return lax.cummax(first, axis=0).astype(jnp.int32)


def draw_in_resp(key, part):
    place = jnp.arange(TOKENS, dtype=jnp.int32)
    device = place // TOK_DEV
    last = max(TOKENS // TOK_DEV - 1, 1)
    threshold = 250 + 500 * device // last
    drawn = jax.random.randint(key, (TOKENS,), 0, 1000)
    chosen = (drawn < threshold) | (place % TOK_DEV == TOK_DEV - 1)
    return chosen.astype(jnp.int32)


def draw_queries(key, part):
    base = jax.random.truncated_normal(jax.random.fold_in(key, 11), -6.0, 6.0, (TOKENS, HEADS * HEAD), jnp.float32)
    return base.astype(jnp.bfloat16)


def draw_keys_values(key, part):
    base = jax.random.truncated_normal(jax.random.fold_in(key, 12), -6.0, 6.0, (TOKENS, 2 * HEAD), jnp.float32)
    return base.astype(jnp.bfloat16)


def with_ends(values, own_key, low, high):
    spot = [jax.random.randint(jax.random.fold_in(own_key, axis), (), 0, length) for axis, length in enumerate(values.shape)]
    widest = values.shape.index(max(values.shape))
    next_to = spot[:widest] + [(spot[widest] + 1) % values.shape[widest]] + spot[widest + 1:]
    return values.at[tuple(spot)].set(low).at[tuple(next_to)].set(high)


def level_of(own_key, extent, cuts, smallest, largest):
    def one(position, parts):
        heights = jax.random.uniform(jax.random.fold_in(jax.random.fold_in(own_key, 6), position), (parts,), jnp.float32, smallest / len(cuts), largest / len(cuts))
        return jnp.repeat(jnp.exp(heights), extent[position] // parts).reshape((-1,) + (1,) * (len(extent) - position - 1))

    gain = one(*cuts[0])
    for cut in cuts[1:]:
        gain = gain * one(*cut)
    return gain


def gaussian(own_key, dims, width, limit, cuts=(), held_as=jnp.bfloat16):
    gain = level_of(own_key, dims, cuts, -0.22, 0.18) if cuts else 1.0
    values = jax.random.normal(own_key, dims, jnp.float32) * width * gain
    return jnp.minimum(jnp.maximum(values, -limit), limit).astype(held_as)


def setup_inputs(seed: int = 0) -> dict:
    key_of = jax.random.split(jax.random.key(seed), 8)
    queries = draw_queries(jax.random.fold_in(key_of[7], 71), 0)
    keys_values = draw_keys_values(jax.random.fold_in(key_of[7], 71), 0)
    seg_ids = draw_seg_ids(jax.random.fold_in(key_of[7], 71), 0)
    in_resp = draw_in_resp(jax.random.fold_in(key_of[7], 71), 0)
    advantage = with_ends(jax.random.randint(key_of[4], (TOKENS,), -24, 25), jax.random.fold_in(key_of[4], 1), -24, 24).astype(jnp.int32)
    out_weight = gaussian(key_of[5], (HEADS * HEAD, D), (HEADS * HEAD) ** -0.5, 0.21875, ((1, 4),))
    upstream = gaussian(key_of[6], (TOKENS, D), 1.0, 6.0, ((0, 32),))
    return {"queries": queries, "keys_values": keys_values, "seg_ids": seg_ids, "in_resp": in_resp, "advantage": advantage, "out_weight": out_weight, "upstream": upstream}


neg_fill = -1.0e30


def attend_forward(q_rows, kv_rows, seg_rows):
    count = q_rows.shape[0]
    head = kv_rows.shape[1] // 2
    heads = q_rows.shape[1] // head
    keys = kv_rows[:, :head]
    values = kv_rows[:, head:]
    place = jnp.arange(count, dtype=jnp.int32)
    allowed = (seg_rows[:, None] == seg_rows[None, :]) & (place[None, :] <= place[:, None])
    scale = head ** -0.5
    outputs = []
    probs = []
    for index in range(heads):
        q_head = q_rows[:, index * head:(index + 1) * head]
        scores = lax.dot_general(q_head, keys, (((1,), (1,)), ((), ())), preferred_element_type=jnp.float32) * scale
        scores = jnp.where(allowed, scores, neg_fill)
        top = jnp.max(scores, axis=1, keepdims=True)
        expo = jnp.exp(scores - top)
        prob = expo / jnp.sum(expo, axis=1, keepdims=True)
        outputs.append(jnp.dot(prob.astype(jnp.bfloat16), values, preferred_element_type=jnp.float32))
        probs.append(prob)
    return jnp.concatenate(outputs, axis=1).astype(jnp.bfloat16), probs


def attend_backward(q_rows, kv_rows, attn_rows, d_attn, probs):
    count = q_rows.shape[0]
    head = kv_rows.shape[1] // 2
    heads = q_rows.shape[1] // head
    keys = kv_rows[:, :head]
    values = kv_rows[:, head:]
    scale = head ** -0.5
    grad_parts = []
    grad_keys = jnp.zeros((count, head), jnp.float32)
    grad_values = jnp.zeros((count, head), jnp.float32)
    for index in range(heads):
        cols = slice(index * head, (index + 1) * head)
        q_head = q_rows[:, cols]
        d_head = d_attn[:, cols]
        delta = jnp.sum(d_head.astype(jnp.float32) * attn_rows[:, cols].astype(jnp.float32), axis=1, keepdims=True)
        d_prob = lax.dot_general(d_head, values, (((1,), (1,)), ((), ())), preferred_element_type=jnp.float32)
        d_score = (probs[index] * (d_prob - delta)).astype(jnp.bfloat16)
        grad_parts.append(jnp.dot(d_score, keys, preferred_element_type=jnp.float32) * scale)
        grad_keys = grad_keys + lax.dot_general(d_score, q_head, (((0,), (0,)), ((), ())), preferred_element_type=jnp.float32) * scale
        grad_values = grad_values + lax.dot_general(probs[index].astype(jnp.bfloat16), d_head, (((0,), (0,)), ((), ())), preferred_element_type=jnp.float32)
    grad_q = jnp.concatenate(grad_parts, axis=1).astype(jnp.bfloat16)
    grad_kv = jnp.concatenate([grad_keys, grad_values], axis=1).astype(jnp.bfloat16)
    return grad_q, grad_kv


def reference(queries, keys_values, seg_ids, in_resp, advantage, out_weight, upstream):
    blocks = TOKENS // TOK_DEV
    resp_total = jnp.sum(in_resp).astype(jnp.float32)
    factor = -(jnp.float32(TOKENS) / resp_total)
    coef = factor * in_resp.astype(jnp.float32) * (advantage.astype(jnp.float32) * 0.125)

    def one_block(total, pieces):
        q_rows, kv_rows, seg_rows, coef_rows, up_rows = pieces
        attn_rows, probs = attend_forward(q_rows, kv_rows, seg_rows)
        branch = jnp.dot(attn_rows, out_weight, preferred_element_type=jnp.float32).astype(jnp.bfloat16)
        d_out = (coef_rows[:, None] * up_rows.astype(jnp.float32)).astype(jnp.bfloat16)
        d_attn = lax.dot_general(d_out, out_weight, (((1,), (1,)), ((), ())), preferred_element_type=jnp.float32).astype(jnp.bfloat16)
        partial_value = lax.dot_general(attn_rows, d_out, (((0,), (0,)), ((), ())), preferred_element_type=jnp.float32).astype(jnp.bfloat16)
        partial_value = lax.optimization_barrier(partial_value)
        grad_q, grad_kv = attend_backward(q_rows, kv_rows, attn_rows, d_attn, probs)
        return total + partial_value.astype(jnp.float32), (branch, grad_q, grad_kv)

    pieces = (queries.reshape(blocks, TOK_DEV, -1), keys_values.reshape(blocks, TOK_DEV, -1),
              seg_ids.reshape(blocks, TOK_DEV), coef.reshape(blocks, TOK_DEV), upstream.reshape(blocks, TOK_DEV, -1))
    start = jnp.zeros(out_weight.shape, jnp.float32)
    grad_weight, (branch, grad_q, grad_kv) = lax.scan(one_block, start, pieces)
    return (branch.reshape(TOKENS, -1), grad_q.reshape(TOKENS, -1), grad_kv.reshape(TOKENS, -1), grad_weight)
```

```python
import functools

import jax
import jax.numpy as jnp
from jax import lax
from jax.experimental import pallas as pl
from jax.experimental.pallas import tpu as pltpu
from jax.sharding import PartitionSpec as P

MESH = pl.DeviceIdType.MESH
neg_fill = -1e30
bf16 = jnp.bfloat16
f32 = jnp.float32
W_CHUNKS = 3


def dot(a, b, dims):
    return lax.dot_general(a, b, ((dims[0], dims[1]), ((), ())), preferred_element_type=f32)


def fused_kernel(
    sizes,
    q_hbm, kv_hbm, seg_hbm, resp_hbm, adv_hbm, w_hbm, up_hbm,
    bo_hbm, gq_hbm, gkv_hbm, gw_hbm,
    q, kv, seg, resp, adv, up,
    w_all, d_out, bo, attn, prob, d_attn, bias, cnt, gq, gkv, gw,
    part, c_recv, x_send, x_recv, z_send, z_recv, y_send, y_recv,
    cnt_y, cnt_z,
    load_sem, out_sem, bo_sem,
    ws_sem, wr_sem, cs_sem, cr_sem, xs_sem, xr_sem, zs_sem, zr_sem, ys_sem, yr_sem,
    ns_sem, nr_sem, nys_sem, nyr_sem, nzs_sem, nzr_sem,
):
    nd, nf, tok, heads, head, rows, cols = sizes
    nz, ny = nd // 2, nf // 2
    half_heads, half_blocks = heads // 2, nd // 2
    scale = head ** (-0.5)
    dp, fs = lax.axis_index("dp"), lax.axis_index("fsdp")
    c, y = lax.rem(fs, 2), lax.div(fs, 2)
    x, z = lax.rem(dp, 2), lax.div(dp, 2)
    sib_f = y * 2 + 1 - c
    sib = (dp, sib_f)
    x_peer = (z * 2 + 1 - x, fs)

    def y_of(j):
        return lax.rem(y + j, ny)

    def z_of(k):
        return lax.rem(z + k, nz)

    def y_dev(j):
        return (dp, y_of(j) * 2 + c)

    def z_dev(k):
        return (z_of(k) * 2 + x, fs)

    def remote(src, dst, ss, rs, dev):
        return pltpu.make_async_remote_copy(
            src_ref=src, dst_ref=dst, send_sem=ss, recv_sem=rs, device_id=dev, device_id_type=MESH
        )

    sends = []

    def send(*args):
        copy = remote(*args)
        copy.start()
        sends.append(copy)

    loads = [
        pltpu.make_async_copy(a, b, load_sem.at[i])
        for i, (a, b) in enumerate(
            [(seg_hbm, seg), (resp_hbm, resp), (adv_hbm, adv), (q_hbm, q), (kv_hbm, kv),
             (up_hbm, up), (w_hbm, w_all.at[fs])]
        )
    ]
    for load in loads:
        load.start()

    barrier = pltpu.get_barrier_semaphore()
    peers = [sib, x_peer] + [y_dev(j) for j in range(1, ny)] + [z_dev(k) for k in range(1, nz)]
    for peer in peers:
        pl.semaphore_signal(barrier, inc=1, device_id=peer, device_id_type=MESH)
    pl.semaphore_wait(barrier, len(peers))

    depth = heads * head
    step = depth // W_CHUNKS

    def w_rows(i):
        return pl.ds(i * step, step)

    for i in range(W_CHUNKS):
        for j in range(1, ny):
            send(w_hbm.at[w_rows(i)], w_all.at[fs, w_rows(i)], ws_sem.at[j, i], wr_sem.at[fs, i], y_dev(j))
    for i in range(W_CHUNKS):
        send(w_hbm.at[w_rows(i)], w_all.at[fs, w_rows(i)], ws_sem.at[0, i], wr_sem.at[fs, i], sib)

    def w_wait(shard, i):
        ref = w_all.at[shard, w_rows(i)]
        remote(ref, ref, ws_sem.at[0, i], wr_sem.at[shard, i], sib).wait_recv()

    def w_forward(i):
        for j in range(1, ny):
            shard = y_of(j) * 2 + c
            w_wait(shard, i)
            send(w_all.at[shard, w_rows(i)], w_all.at[shard, w_rows(i)],
                 ws_sem.at[ny - 1 + j, i], wr_sem.at[shard, i], sib)

    for load in loads[:3]:
        load.wait()
    count = jnp.sum(resp[...].astype(f32), axis=1, keepdims=True)
    cnt[0] = jnp.broadcast_to(count, cnt.shape[1:])
    coef_row = resp[...].astype(f32) * (adv[...].astype(f32) * 0.125)
    coef = jnp.transpose(jnp.broadcast_to(coef_row, (128, tok)))[:, :1]
    seg_k = jnp.broadcast_to(seg[...].astype(f32), (tok, tok))
    seg_q = jnp.transpose(seg_k)
    at_q = lax.broadcasted_iota(jnp.int32, (tok, tok), 0)
    at_k = lax.broadcasted_iota(jnp.int32, (tok, tok), 1)
    bias[...] = jnp.where((seg_q == seg_k) & (at_k <= at_q), 0.0, neg_fill)
    send(cnt.at[0], cnt.at[1], ns_sem.at[0], nr_sem.at[0], sib)
    for load in loads[3:6]:
        load.wait()
    for s in range(nf):
        d_out[s] = (coef * up[:, s * cols:(s + 1) * cols].astype(f32)).astype(bf16)
    keys, values = kv[:, :head], kv[:, head:]

    def forward(h):
        cut = slice(h * head, (h + 1) * head)
        scores = dot(q[:, cut], keys, ((1,), (1,))) * scale + bias[...]
        top = jnp.max(scores, axis=1, keepdims=True)
        expo = jnp.exp(scores - top)
        p = (expo * (1.0 / jnp.sum(expo, axis=1, keepdims=True))).astype(bf16)
        prob[h] = p
        attn[:, cut] = dot(p, values, ((1,), (0,))).astype(bf16)

    def partial(hf):
        width = half_heads * head
        left = attn[:, hf * width:(hf + 1) * width]
        for s in range(nf):
            got = dot(left, d_out[s], ((0,), (0,))).astype(bf16)
            for b in range(half_blocks):
                part[s, hf * half_blocks + b] = got[b * rows:(b + 1) * rows]
        blocks = pl.ds(hf * half_blocks, half_blocks)
        for j in range(1, ny + 1):
            yy = y_of(j)
            send(part.at[yy * 2 + 1 - c, blocks], c_recv.at[yy, blocks],
                 cs_sem.at[hf, yy], cr_sem.at[hf, yy], sib)

    def c_stage(hf):
        blocks = pl.ds(hf * half_blocks, half_blocks)
        for j in range(1, ny + 1):
            yy = y_of(j)
            ref = c_recv.at[yy, blocks]
            remote(ref, ref, cs_sem.at[hf, yy], cr_sem.at[hf, yy], sib).wait_recv()
            for zz in range(hf * nz // 2, (hf + 1) * nz // 2):
                block = zz * 2 + 1 - x
                both = part[yy * 2 + c, block].astype(f32) + c_recv[yy, block].astype(f32)
                x_send[zz, yy] = both.astype(bf16)
                send(x_send.at[zz, yy], x_recv.at[zz, yy], xs_sem.at[zz, yy], xr_sem.at[zz, yy], x_peer)

    def x_stage(zz, j):
        yy = y_of(j)
        ref = x_recv.at[zz, yy]
        remote(ref, ref, xs_sem.at[zz, yy], xr_sem.at[zz, yy], x_peer).wait_recv()
        block = zz * 2 + x
        total = part[yy * 2 + c, block].astype(f32) + c_recv[yy, block].astype(f32) + ref[...].astype(f32)
        z_send[zz, yy] = total.astype(bf16)

        @pl.when(zz != z)
        def _():
            remote(z_send.at[zz, yy], z_recv.at[z, yy], zs_sem.at[zz, yy], zr_sem.at[z, yy],
                   (zz * 2 + x, fs)).start()

    def z_stage(j):
        yy = y_of(j)
        total = z_send[z, yy].astype(f32)
        for k in range(1, nz):
            src = z_of(k)
            ref = z_recv.at[src, yy]
            remote(ref, ref, zs_sem.at[src, yy], zr_sem.at[src, yy], z_dev(k)).wait_recv()
            total = total + ref[...].astype(f32)
        return total

    def use_weight(s, first=False):
        w = w_all[s]
        bo[s] = dot(attn[...], w, ((1,), (0,))).astype(bf16)
        pltpu.make_async_copy(
            bo.at[s], bo_hbm.at[:, pl.ds(pl.multiple_of(s * cols, 128), cols)], bo_sem.at[s]
        ).start()
        grad = dot(d_out[s], w, ((1,), (1,)))
        d_attn[...] = grad if first else d_attn[...] + grad

    def count_core():
        remote(cnt.at[1], cnt.at[1], ns_sem.at[0], nr_sem.at[0], sib).wait_recv()
        cnt[2] = cnt[0] + cnt[1]
        for j in range(1, ny):
            send(cnt.at[2], cnt_y.at[y], nys_sem.at[j], nyr_sem.at[y], y_dev(j))

    def count_y():
        total = cnt[2]
        for j in range(1, ny):
            ref = cnt_y.at[y_of(j)]
            remote(ref, ref, nys_sem.at[j], nyr_sem.at[y_of(j)], y_dev(j)).wait_recv()
            total = total + ref[...]
        cnt[3] = total
        send(cnt.at[3], cnt.at[4], ns_sem.at[1], nr_sem.at[1], x_peer)

    def count_x():
        remote(cnt.at[4], cnt.at[4], ns_sem.at[1], nr_sem.at[1], x_peer).wait_recv()
        cnt[5] = cnt[3] + cnt[4]
        for k in range(1, nz):
            send(cnt.at[5], cnt_z.at[z], nzs_sem.at[k], nzr_sem.at[z], z_dev(k))

    def count_z():
        total = cnt[5]
        for k in range(1, nz):
            ref = cnt_z.at[z_of(k)]
            remote(ref, ref, nzs_sem.at[k], nzr_sem.at[z_of(k)], z_dev(k)).wait_recv()
            total = total + ref[...]
        return -(f32(tok * nd * nf) / total[:1, :1])

    for h in range(half_heads):
        forward(h)
    partial(0)
    for h in range(half_heads, heads):
        forward(h)
    count_core()
    partial(1)
    c_stage(0)
    count_y()
    loads[6].wait()
    c_stage(1)
    use_weight(fs, first=True)
    w_forward(0)
    for i in range(W_CHUNKS):
        w_wait(sib_f, i)
    use_weight(sib_f)
    count_x()

    state = {}

    def weights_of(j):
        shard = y_of(j) * 2 + c
        use_weight(shard)

    def weights_other(j):
        shard = y_of(j) * 2 + 1 - c
        for i in range(W_CHUNKS):
            w_wait(shard, i)
        use_weight(shard)

    def backward(h):
        if h == 0:
            state["factor"] = count_z()
            state["gk"] = jnp.zeros((tok, head), f32)
            state["gv"] = jnp.zeros((tok, head), f32)
        factor = state["factor"]
        cut = slice(h * head, (h + 1) * head)
        d_full = d_attn[:, cut]
        d_head = d_full.astype(bf16)
        delta = jnp.sum(d_head.astype(f32) * attn[:, cut].astype(f32), axis=1, keepdims=True)
        p = prob[h]
        d_prob = dot(d_head, values, ((1,), (1,)))
        d_score = (p.astype(f32) * (d_prob - delta)).astype(bf16)
        gq[:, cut] = (dot(d_score, keys, ((1,), (0,))) * (scale * factor)).astype(bf16)
        state["gk"] = state["gk"] + dot(d_score, q[:, cut], ((0,), (0,)))
        state["gv"] = state["gv"] + dot(p, d_head, ((0,), (0,)))
        if h == heads - 1:
            gkv[:, :head] = (state["gk"] * (scale * factor)).astype(bf16)
            gkv[:, head:] = (state["gv"] * factor).astype(bf16)
            pltpu.make_async_copy(gq, gq_hbm, out_sem.at[0]).start()
            pltpu.make_async_copy(gkv, gkv_hbm, out_sem.at[1]).start()

    x_steps = [
        functools.partial(x_stage, zz, j)
        for hf in range(2)
        for j in range(1, ny + 1)
        for zz in range(hf * nz // 2, (hf + 1) * nz // 2)
    ]
    fillers = [functools.partial(w_forward, i) for i in range(1, W_CHUNKS)]
    fillers += [functools.partial(weights_of, j) for j in range(1, ny)]
    fillers += [functools.partial(weights_other, j) for j in range(1, ny)]
    fillers += [functools.partial(backward, h) for h in range(heads)]
    done = 0
    for n, x_step in enumerate(x_steps):
        x_step()
        until = (n + 1) * len(fillers) // len(x_steps)
        for filler in fillers[done:until]:
            filler()
        done = until

    factor = state["factor"]
    for j in range(1, ny):
        y_send[j - 1] = z_stage(j).astype(bf16)
        send(y_send.at[j - 1], y_recv.at[y], ys_sem.at[j - 1], yr_sem.at[y], y_dev(j))
    total = z_stage(ny)
    for j in range(1, ny):
        src = y_of(j)
        ref = y_recv.at[src]
        remote(ref, ref, ys_sem.at[j - 1], yr_sem.at[src], y_dev(j)).wait_recv()
        total = total + ref[...].astype(f32)
    gw[...] = total * factor
    pltpu.make_async_copy(gw, gw_hbm, out_sem.at[2]).start()

    for copy in sends:
        copy.wait_send()
    for zz in range(nz):
        for yy in range(ny):
            @pl.when(zz != z)
            def _(zz=zz, yy=yy):
                remote(z_send.at[zz, yy], z_recv.at[z, yy], zs_sem.at[zz, yy], zr_sem.at[z, yy],
                       (zz * 2 + x, fs)).wait_send()
    for s in range(nf):
        pltpu.make_async_copy(bo.at[s], bo_hbm.at[:, pl.ds(s * cols, cols)], bo_sem.at[s]).wait()
    pltpu.make_async_copy(gq, gq_hbm, out_sem.at[0]).wait()
    pltpu.make_async_copy(gkv, gkv_hbm, out_sem.at[1]).wait()
    pltpu.make_async_copy(gw, gw_hbm, out_sem.at[2]).wait()


def fused(nd, nf, queries, keys_values, seg_ids, in_resp, advantage, out_weight, upstream):
    tok, depth = queries.shape
    head = keys_values.shape[1] // 2
    heads = depth // head
    cols = out_weight.shape[1]
    rows = depth // nd
    nz, ny = nd // 2, nf // 2
    any_spec = pl.BlockSpec(memory_space=pl.ANY)
    V, D = pltpu.VMEM, pltpu.SemaphoreType.DMA
    return pl.pallas_call(
        functools.partial(fused_kernel, (nd, nf, tok, heads, head, rows, cols)),
        out_shape=(
            jax.ShapeDtypeStruct((tok, nf * cols), bf16),
            jax.ShapeDtypeStruct((tok, depth), bf16),
            jax.ShapeDtypeStruct((tok, 2 * head), bf16),
            jax.ShapeDtypeStruct((rows, cols), f32),
        ),
        in_specs=[any_spec] * 7,
        out_specs=(any_spec,) * 4,
        scratch_shapes=[
            V((tok, depth), bf16), V((tok, 2 * head), bf16),
            V((1, tok), jnp.int32), V((1, tok), jnp.int32), V((1, tok), jnp.int32),
            V((tok, nf * cols), bf16),
            V((nf, depth, cols), bf16), V((nf, tok, cols), bf16), V((nf, tok, cols), bf16),
            V((tok, depth), bf16), V((heads, tok, tok), bf16), V((tok, depth), f32),
            V((tok, tok), f32), V((6, 8, 128), f32),
            V((tok, depth), bf16), V((tok, 2 * head), bf16), V((rows, cols), f32),
            V((nf, nd, rows, cols), bf16), V((ny, nd, rows, cols), bf16),
            V((nz, ny, rows, cols), bf16), V((nz, ny, rows, cols), bf16),
            V((nz, ny, rows, cols), bf16), V((nz, ny, rows, cols), bf16),
            V((ny, rows, cols), bf16), V((ny, rows, cols), bf16),
            V((ny, 8, 128), f32), V((nz, 8, 128), f32),
            D((7,)), D((3,)), D((nf,)),
            D((nf, W_CHUNKS)), D((nf, W_CHUNKS)),
            D((2, ny)), D((2, ny)), D((nz, ny)), D((nz, ny)), D((nz, ny)), D((nz, ny)),
            D((ny,)), D((ny,)),
            D((2,)), D((2,)), D((ny,)), D((ny,)), D((nz,)), D((nz,)),
        ],
        compiler_params=pltpu.CompilerParams(
            collective_id=0, has_side_effects=True, vmem_limit_bytes=48 * 1024 * 1024
        ),
    )(
        queries, keys_values, seg_ids.reshape(1, -1), in_resp.reshape(1, -1),
        advantage.reshape(1, -1), out_weight, upstream,
    )


def attend_forward(q_rows, kv_rows, seg_rows):
    count = q_rows.shape[0]
    head = kv_rows.shape[1] // 2
    heads = q_rows.shape[1] // head
    keys = kv_rows[:, :head]
    values = kv_rows[:, head:]
    place = jnp.arange(count, dtype=jnp.int32)
    allowed = (seg_rows[:, None] == seg_rows[None, :]) & (place[None, :] <= place[:, None])
    scale = head ** (-0.5)
    outputs = []
    probs = []
    for index in range(heads):
        q_head = q_rows[:, index * head : (index + 1) * head]
        scores = (
            lax.dot_general(
                q_head, keys, (((1,), (1,)), ((), ())), preferred_element_type=jnp.float32
            )
            * scale
        )
        scores = jnp.where(allowed, scores, neg_fill)
        top = jnp.max(scores, axis=1, keepdims=True)
        expo = jnp.exp(scores - top)
        prob = expo / jnp.sum(expo, axis=1, keepdims=True)
        outputs.append(
            jnp.dot(prob.astype(jnp.bfloat16), values, preferred_element_type=jnp.float32)
        )
        probs.append(prob)
    return (jnp.concatenate(outputs, axis=1).astype(jnp.bfloat16), probs)


def attend_backward(q_rows, kv_rows, attn_rows, d_attn, probs):
    count = q_rows.shape[0]
    head = kv_rows.shape[1] // 2
    heads = q_rows.shape[1] // head
    keys = kv_rows[:, :head]
    values = kv_rows[:, head:]
    scale = head ** (-0.5)
    grad_parts = []
    grad_keys = jnp.zeros((count, head), jnp.float32)
    grad_values = jnp.zeros((count, head), jnp.float32)
    for index in range(heads):
        cols = slice(index * head, (index + 1) * head)
        q_head = q_rows[:, cols]
        d_head = d_attn[:, cols]
        delta = jnp.sum(
            d_head.astype(jnp.float32) * attn_rows[:, cols].astype(jnp.float32),
            axis=1,
            keepdims=True,
        )
        d_prob = lax.dot_general(
            d_head, values, (((1,), (1,)), ((), ())), preferred_element_type=jnp.float32
        )
        d_score = (probs[index] * (d_prob - delta)).astype(jnp.bfloat16)
        grad_parts.append(jnp.dot(d_score, keys, preferred_element_type=jnp.float32) * scale)
        grad_keys = (
            grad_keys
            + lax.dot_general(
                d_score, q_head, (((0,), (0,)), ((), ())), preferred_element_type=jnp.float32
            )
            * scale
        )
        grad_values = grad_values + lax.dot_general(
            probs[index].astype(jnp.bfloat16),
            d_head,
            (((0,), (0,)), ((), ())),
            preferred_element_type=jnp.float32,
        )
    grad_q = jnp.concatenate(grad_parts, axis=1).astype(jnp.bfloat16)
    grad_kv = jnp.concatenate([grad_keys, grad_values], axis=1).astype(jnp.bfloat16)
    return (grad_q, grad_kv)


def on_device(queries, keys_values, seg_ids, in_resp, advantage, out_weight, upstream):
    attn_rows, probs = attend_forward(queries, keys_values, seg_ids)
    whole_weight = lax.all_gather(out_weight, "fsdp", axis=1, tiled=True)
    branch = jnp.dot(attn_rows, whole_weight, preferred_element_type=jnp.float32)
    branch_out = branch.astype(jnp.bfloat16)
    resp_total = lax.psum(jnp.sum(in_resp), ("dp", "fsdp"))
    all_tokens = queries.shape[0] * lax.axis_size("dp") * lax.axis_size("fsdp")
    factor = -(jnp.float32(all_tokens) / resp_total.astype(jnp.float32))
    coef = factor * in_resp.astype(jnp.float32) * (advantage.astype(jnp.float32) * 0.125)
    d_out = (coef[:, None] * upstream.astype(jnp.float32)).astype(jnp.bfloat16)
    d_attn = lax.dot_general(
        d_out, whole_weight, (((1,), (1,)), ((), ())), preferred_element_type=jnp.float32
    )
    d_attn = d_attn.astype(jnp.bfloat16)
    partial_value = lax.dot_general(
        attn_rows, d_out, (((0,), (0,)), ((), ())), preferred_element_type=jnp.float32
    )
    column_sums = lax.psum_scatter(
        partial_value.astype(jnp.bfloat16), "fsdp", scatter_dimension=1, tiled=True
    ).astype(jnp.float32)
    grad_weight = lax.psum_scatter(column_sums, "dp", scatter_dimension=0, tiled=True)
    grad_q, grad_kv = attend_backward(queries, keys_values, attn_rows, d_attn, probs)
    return (branch_out, grad_q, grad_kv, grad_weight)


def solution(mesh):
    in_specs = (
        P(("dp", "fsdp"), None),
        P(("dp", "fsdp"), None),
        P(("dp", "fsdp")),
        P(("dp", "fsdp")),
        P(("dp", "fsdp")),
        P(None, "fsdp"),
        P(("dp", "fsdp"), None),
    )
    out_specs = (
        P(("dp", "fsdp"), None),
        P(("dp", "fsdp"), None),
        P(("dp", "fsdp"), None),
        P("dp", "fsdp"),
    )
    nd, nf = mesh.shape["dp"], mesh.shape["fsdp"]

    def on_each(queries, keys_values, seg_ids, in_resp, advantage, out_weight, upstream):
        args = (queries, keys_values, seg_ids, in_resp, advantage, out_weight, upstream)
        depth, cols = out_weight.shape
        head = keys_values.shape[1] // 2
        heads = depth // head
        fits = (
            nd % 4 == 0 and nf % 2 == 0 and heads % 2 == 0 and depth % (16 * nd) == 0
            and cols % 128 == 0 and head % 128 == 0 and depth % (16 * W_CHUNKS) == 0
        )
        if fits:
            return fused(nd, nf, *args)
        return on_device(*args)

    return jax.shard_map(
        on_each, mesh=mesh, in_specs=in_specs, out_specs=out_specs, check_vma=False
    )
```

```python
import functools

import jax
import jax.numpy as jnp
from jax import lax
from jax.experimental import pallas as pl
from jax.experimental.pallas import tpu as pltpu
from jax.sharding import PartitionSpec as P

MESH = pl.DeviceIdType.MESH
neg_fill = -1e30
bf16 = jnp.bfloat16
f32 = jnp.float32
W_CHUNKS = 3


def dot(a, b, dims):
    return lax.dot_general(a, b, ((dims[0], dims[1]), ((), ())), preferred_element_type=f32)


def fused_kernel(
    sizes,
    q_hbm, kv_hbm, seg_hbm, resp_hbm, adv_hbm, w_hbm, up_hbm,
    bo, gq, gkv, gw,
    q, kv, seg, resp, adv, up,
    w_all, d_out, attn, prob, d_attn, bias, cnt,
    part, c_recv, x_send, x_recv, z_send, z_recv, y_send, y_recv,
    cnt_y, cnt_z,
    load_sem,
    ws_sem, wr_sem, cs_sem, cr_sem, xs_sem, xr_sem, zs_sem, zr_sem, ys_sem, yr_sem,
    ns_sem, nr_sem, nys_sem, nyr_sem, nzs_sem, nzr_sem,
):
    nd, nf, tok, heads, head, rows, cols = sizes
    nz, ny = nd // 2, nf // 2
    half_heads, half_blocks, half_z = heads // 2, nd // 2, nz // 2
    scale = head ** (-0.5)
    dp, fs = lax.axis_index("dp"), lax.axis_index("fsdp")
    c, y = lax.rem(fs, 2), lax.div(fs, 2)
    x, z = lax.rem(dp, 2), lax.div(dp, 2)
    sib_f = y * 2 + 1 - c
    sib = (dp, sib_f)
    x_peer = (z * 2 + 1 - x, fs)

    far = 1 - lax.div(z, half_z)
    halves = (far, 1 - far)

    def owners(n):
        base = halves[n] * half_z
        if n == 0:
            return [base + i for i in range(half_z)]
        return [base + lax.rem(z - base + 1 + i, half_z) for i in range(half_z)]

    def y_of(j):
        return lax.rem(y + j, ny)

    def z_of(k):
        return lax.rem(z + k, nz)

    def y_dev(j):
        return (dp, y_of(j) * 2 + c)

    def z_dev(k):
        return (z_of(k) * 2 + x, fs)

    def remote(src, dst, ss, rs, dev):
        return pltpu.make_async_remote_copy(
            src_ref=src, dst_ref=dst, send_sem=ss, recv_sem=rs, device_id=dev, device_id_type=MESH
        )

    sends = []

    def send(*args):
        copy = remote(*args)
        copy.start()
        sends.append(copy)

    loads = [
        pltpu.make_async_copy(a, b, load_sem.at[i])
        for i, (a, b) in enumerate(
            [(seg_hbm, seg), (resp_hbm, resp), (adv_hbm, adv), (q_hbm, q), (kv_hbm, kv),
             (up_hbm, up), (w_hbm, w_all.at[fs])]
        )
    ]
    for load in loads:
        load.start()

    loads[1].wait()
    count = jnp.sum(resp[...].astype(f32), axis=1, keepdims=True)
    cnt[0] = jnp.broadcast_to(count, cnt.shape[1:])

    barrier = pltpu.get_barrier_semaphore()
    peers = [sib, x_peer] + [y_dev(j) for j in range(1, ny)] + [z_dev(k) for k in range(1, nz)]
    for peer in peers:
        pl.semaphore_signal(barrier, inc=1, device_id=peer, device_id_type=MESH)
    pl.semaphore_wait(barrier, len(peers))
    for j in range(1, ny):
        send(cnt.at[0], cnt_y.at[y], nys_sem.at[j], nyr_sem.at[y], y_dev(j))

    depth = heads * head
    step = depth // W_CHUNKS

    def w_rows(i):
        return pl.ds(i * step, step)

    for i in range(W_CHUNKS):
        for j in range(1, ny):
            send(w_hbm.at[w_rows(i)], w_all.at[fs, w_rows(i)], ws_sem.at[j, i], wr_sem.at[fs, i], y_dev(j))
    for i in range(W_CHUNKS):
        send(w_hbm.at[w_rows(i)], w_all.at[fs, w_rows(i)], ws_sem.at[0, i], wr_sem.at[fs, i], sib)

    def w_wait(shard, i):
        ref = w_all.at[shard, w_rows(i)]
        remote(ref, ref, ws_sem.at[0, i], wr_sem.at[shard, i], sib).wait_recv()

    def w_forward(i):
        for j in range(1, ny):
            shard = y_of(j) * 2 + c
            w_wait(shard, i)
            send(w_all.at[shard, w_rows(i)], w_all.at[shard, w_rows(i)],
                 ws_sem.at[ny - 1 + j, i], wr_sem.at[shard, i], sib)

    for load in (loads[0], loads[2]):
        load.wait()
    coef_row = resp[...].astype(f32) * (adv[...].astype(f32) * 0.125)
    coef = jnp.transpose(jnp.broadcast_to(coef_row, (128, tok)))[:, :1]
    seg_k = jnp.broadcast_to(seg[...].astype(f32), (tok, tok))
    seg_q = jnp.transpose(seg_k)
    at_q = lax.broadcasted_iota(jnp.int32, (tok, tok), 0)
    at_k = lax.broadcasted_iota(jnp.int32, (tok, tok), 1)
    bias[...] = jnp.where((seg_q == seg_k) & (at_k <= at_q), 0.0, neg_fill)
    for load in loads[3:6]:
        load.wait()
    for s in range(nf):
        d_out[s] = (coef * up[:, s * cols:(s + 1) * cols].astype(f32)).astype(bf16)
    keys, values = kv[:, :head], kv[:, head:]

    def lanes(h):
        return pl.ds(pl.multiple_of(h * head, 128), head)

    def forward(h):
        cut = lanes(h)
        scores = dot(q[:, cut], keys, ((1,), (1,))) * scale + bias[...]
        top = jnp.max(scores, axis=1, keepdims=True)
        expo = jnp.exp(scores - top)
        p = (expo * (1.0 / jnp.sum(expo, axis=1, keepdims=True))).astype(bf16)
        prob[h] = p
        attn[:, cut] = dot(p, values, ((1,), (0,))).astype(bf16)

    def partial(n):
        width = half_heads * head
        left = attn[:, pl.ds(pl.multiple_of(halves[n] * width, 128), width)]
        first = halves[n] * half_blocks
        blocks = pl.ds(first, half_blocks)

        def shard(s):
            got = dot(left, d_out[s], ((0,), (0,))).astype(bf16)
            for b in range(half_blocks):
                part[s, first + b] = got[b * rows:(b + 1) * rows]

        for j in range(1, ny + 1):
            yy = y_of(j)
            shard(yy * 2 + 1 - c)
            send(part.at[yy * 2 + 1 - c, blocks], c_recv.at[yy, blocks],
                 cs_sem.at[n, yy], cr_sem.at[n, yy], sib)
        for j in range(1, ny + 1):
            shard(y_of(j) * 2 + c)

    def x_order(n):
        zs = owners(n)
        return [(zz, j, n == 0 or zz is not zs[-1]) for j in range(1, ny + 1) for zz in zs]

    def c_stage(n):
        blocks = pl.ds(halves[n] * half_blocks, half_blocks)
        waited = set()
        for zz, j, _ in x_order(n):
            yy = y_of(j)
            if j not in waited:
                waited.add(j)
                ref = c_recv.at[yy, blocks]
                remote(ref, ref, cs_sem.at[n, yy], cr_sem.at[n, yy], sib).wait_recv()
            block = zz * 2 + 1 - x
            both = part[yy * 2 + c, block].astype(f32) + c_recv[yy, block].astype(f32)
            x_send[zz, yy] = both.astype(bf16)
            send(x_send.at[zz, yy], x_recv.at[zz, yy], xs_sem.at[zz, yy], xr_sem.at[zz, yy], x_peer)

    def x_stage(zz, j, leaves):
        yy = y_of(j)
        ref = x_recv.at[zz, yy]
        remote(ref, ref, xs_sem.at[zz, yy], xr_sem.at[zz, yy], x_peer).wait_recv()
        block = zz * 2 + x
        total = part[yy * 2 + c, block].astype(f32) + c_recv[yy, block].astype(f32) + ref[...].astype(f32)
        z_send[zz, yy] = total.astype(bf16)
        if leaves:
            send(z_send.at[zz, yy], z_recv.at[z, yy], zs_sem.at[zz, yy], zr_sem.at[z, yy],
                 (zz * 2 + x, fs))

    def z_stage(j):
        yy = y_of(j)
        total = z_send[z, yy].astype(f32)
        for k in range(1, nz):
            src = z_of(k)
            ref = z_recv.at[src, yy]
            remote(ref, ref, zs_sem.at[src, yy], zr_sem.at[src, yy], z_dev(k)).wait_recv()
            total = total + ref[...].astype(f32)
        return total

    def use_weight(s, first=False):
        w = w_all[s]
        bo[:, pl.ds(pl.multiple_of(s * cols, 128), cols)] = dot(attn[...], w, ((1,), (0,))).astype(bf16)
        grad = dot(d_out[s], w, ((1,), (1,)))
        d_attn[...] = grad if first else d_attn[...] + grad

    def count_y():
        total = cnt[0]
        for j in range(1, ny):
            ref = cnt_y.at[y_of(j)]
            remote(ref, ref, nys_sem.at[j], nyr_sem.at[y_of(j)], y_dev(j)).wait_recv()
            total = total + ref[...]
        cnt[1] = total
        send(cnt.at[1], cnt.at[2], ns_sem.at[0], nr_sem.at[0], sib)

    def count_core():
        remote(cnt.at[2], cnt.at[2], ns_sem.at[0], nr_sem.at[0], sib).wait_recv()
        cnt[3] = cnt[1] + cnt[2]
        send(cnt.at[3], cnt.at[4], ns_sem.at[1], nr_sem.at[1], x_peer)

    def count_x():
        remote(cnt.at[4], cnt.at[4], ns_sem.at[1], nr_sem.at[1], x_peer).wait_recv()
        cnt[5] = cnt[3] + cnt[4]
        for k in range(1, nz):
            send(cnt.at[5], cnt_z.at[z], nzs_sem.at[k], nzr_sem.at[z], z_dev(k))

    def count_z():
        total = cnt[5]
        for k in range(1, nz):
            ref = cnt_z.at[z_of(k)]
            remote(ref, ref, nzs_sem.at[k], nzr_sem.at[z_of(k)], z_dev(k)).wait_recv()
            total = total + ref[...]
        return -(f32(tok * nd * nf) / total[:1, :1])

    for i in range(half_heads):
        forward(halves[0] * half_heads + i)
    count_y()
    partial(0)
    count_core()
    for i in range(half_heads):
        forward(halves[1] * half_heads + i)
    c_stage(0)
    partial(1)
    count_x()
    c_stage(1)
    loads[6].wait()
    use_weight(fs, first=True)
    w_forward(0)
    for i in range(W_CHUNKS):
        w_wait(sib_f, i)
    use_weight(sib_f)

    state = {}

    def weights_of(j):
        shard = y_of(j) * 2 + c
        use_weight(shard)

    def weights_other(j):
        shard = y_of(j) * 2 + 1 - c
        for i in range(W_CHUNKS):
            w_wait(shard, i)
        use_weight(shard)

    def backward(h):
        if h == 0:
            state["factor"] = count_z()
            state["gk"] = jnp.zeros((tok, head), f32)
            state["gv"] = jnp.zeros((tok, head), f32)
        factor = state["factor"]
        cut = slice(h * head, (h + 1) * head)
        d_full = d_attn[:, cut]
        d_head = d_full.astype(bf16)
        delta = jnp.sum(d_head.astype(f32) * attn[:, cut].astype(f32), axis=1, keepdims=True)
        p = prob[h]
        d_prob = dot(d_head, values, ((1,), (1,)))
        d_score = (p.astype(f32) * (d_prob - delta)).astype(bf16)
        gq[:, cut] = (dot(d_score, keys, ((1,), (0,))) * (scale * factor)).astype(bf16)
        state["gk"] = state["gk"] + dot(d_score, q[:, cut], ((0,), (0,)))
        state["gv"] = state["gv"] + dot(p, d_head, ((0,), (0,)))
        if h == heads - 1:
            gkv[:, :head] = (state["gk"] * (scale * factor)).astype(bf16)
            gkv[:, head:] = (state["gv"] * factor).astype(bf16)

    fillers = [functools.partial(w_forward, i) for i in range(1, W_CHUNKS)]
    fillers += [functools.partial(weights_of, j) for j in range(1, ny)]
    fillers += [functools.partial(weights_other, j) for j in range(1, ny)]
    fillers += [functools.partial(backward, h) for h in range(heads)]
    x_steps = [item for n in range(2) for item in x_order(n)]
    slots = len(x_steps) - half_z
    done = 0
    for n, x_step in enumerate(x_steps):
        x_stage(*x_step)
        until = (n + 1) * len(fillers) // slots
        for filler in fillers[done:until]:
            filler()
        done = max(done, until)
        passed = n + 1 - ny * half_z
        if passed > 0 and passed % half_z == 0 and passed < ny * half_z:
            j = passed // half_z
            y_send[j - 1] = z_stage(j).astype(bf16)
            send(y_send.at[j - 1], y_recv.at[y], ys_sem.at[j - 1], yr_sem.at[y], y_dev(j))

    factor = state["factor"]
    total = z_stage(ny)
    for j in range(1, ny):
        src = y_of(j)
        ref = y_recv.at[src]
        remote(ref, ref, ys_sem.at[j - 1], yr_sem.at[src], y_dev(j)).wait_recv()
        total = total + ref[...].astype(f32)
    gw[...] = total * factor

    for copy in sends:
        copy.wait_send()


def copy_out(a, b, c, d, a_hbm, b_hbm, c_hbm, d_hbm, sem):
    pairs = [(a, a_hbm), (b, b_hbm), (c, c_hbm), (d, d_hbm)]
    copies = [pltpu.make_async_copy(*pair, sem.at[i]) for i, pair in enumerate(pairs)]
    for copy in copies:
        copy.start()
    for copy in copies:
        copy.wait()


def fused(nd, nf, queries, keys_values, seg_ids, in_resp, advantage, out_weight, upstream):
    tok, depth = queries.shape
    head = keys_values.shape[1] // 2
    heads = depth // head
    cols = out_weight.shape[1]
    rows = depth // nd
    nz, ny = nd // 2, nf // 2
    hbm_spec = pl.BlockSpec(memory_space=pltpu.HBM)
    any_spec = pl.BlockSpec(memory_space=pl.ANY)
    V, D = pltpu.VMEM, pltpu.SemaphoreType.DMA
    results = pl.pallas_call(
        functools.partial(fused_kernel, (nd, nf, tok, heads, head, rows, cols)),
        out_shape=(
            pltpu.VMEM((tok, nf * cols), bf16),
            pltpu.VMEM((tok, depth), bf16),
            pltpu.VMEM((tok, 2 * head), bf16),
            pltpu.VMEM((rows, cols), f32),
        ),
        in_specs=[hbm_spec] * 7,
        out_specs=(pl.BlockSpec(memory_space=pltpu.VMEM),) * 4,
        scratch_shapes=[
            V((tok, depth), bf16), V((tok, 2 * head), bf16),
            V((1, tok), jnp.int32), V((1, tok), jnp.int32), V((1, tok), jnp.int32),
            V((tok, nf * cols), bf16),
            V((nf, depth, cols), bf16), V((nf, tok, cols), bf16),
            V((tok, depth), bf16), V((heads, tok, tok), bf16), V((tok, depth), f32),
            V((tok, tok), f32), V((6, 8, 128), f32),
            V((nf, nd, rows, cols), bf16), V((ny, nd, rows, cols), bf16),
            V((nz, ny, rows, cols), bf16), V((nz, ny, rows, cols), bf16),
            V((nz, ny, rows, cols), bf16), V((nz, ny, rows, cols), bf16),
            V((ny, rows, cols), bf16), V((ny, rows, cols), bf16),
            V((ny, 8, 128), f32), V((nz, 8, 128), f32),
            D((7,)),
            D((nf, W_CHUNKS)), D((nf, W_CHUNKS)),
            D((2, ny)), D((2, ny)), D((nz, ny)), D((nz, ny)), D((nz, ny)), D((nz, ny)),
            D((ny,)), D((ny,)),
            D((2,)), D((2,)), D((ny,)), D((ny,)), D((nz,)), D((nz,)),
        ],
        compiler_params=pltpu.CompilerParams(
            collective_id=0, has_side_effects=True, vmem_limit_bytes=60 * 1024 * 1024
        ),
    )(
        *[pltpu.with_memory_space_constraint(a, pltpu.HBM) for a in (
            queries, keys_values, seg_ids.reshape(1, -1), in_resp.reshape(1, -1),
            advantage.reshape(1, -1), out_weight, upstream,
        )]
    )
    return pl.pallas_call(
        copy_out,
        out_shape=tuple(pltpu.HBM(r.shape, r.dtype) for r in results),
        in_specs=[pl.BlockSpec(memory_space=pltpu.VMEM)] * 4,
        out_specs=(any_spec,) * 4,
        scratch_shapes=[D((4,))],
        compiler_params=pltpu.CompilerParams(vmem_limit_bytes=4 * 1024 * 1024),
    )(*results)


def attend_forward(q_rows, kv_rows, seg_rows):
    count = q_rows.shape[0]
    head = kv_rows.shape[1] // 2
    heads = q_rows.shape[1] // head
    keys = kv_rows[:, :head]
    values = kv_rows[:, head:]
    place = jnp.arange(count, dtype=jnp.int32)
    allowed = (seg_rows[:, None] == seg_rows[None, :]) & (place[None, :] <= place[:, None])
    scale = head ** (-0.5)
    outputs = []
    probs = []
    for index in range(heads):
        q_head = q_rows[:, index * head : (index + 1) * head]
        scores = (
            lax.dot_general(
                q_head, keys, (((1,), (1,)), ((), ())), preferred_element_type=jnp.float32
            )
            * scale
        )
        scores = jnp.where(allowed, scores, neg_fill)
        top = jnp.max(scores, axis=1, keepdims=True)
        expo = jnp.exp(scores - top)
        prob = expo / jnp.sum(expo, axis=1, keepdims=True)
        outputs.append(
            jnp.dot(prob.astype(jnp.bfloat16), values, preferred_element_type=jnp.float32)
        )
        probs.append(prob)
    return (jnp.concatenate(outputs, axis=1).astype(jnp.bfloat16), probs)


def attend_backward(q_rows, kv_rows, attn_rows, d_attn, probs):
    count = q_rows.shape[0]
    head = kv_rows.shape[1] // 2
    heads = q_rows.shape[1] // head
    keys = kv_rows[:, :head]
    values = kv_rows[:, head:]
    scale = head ** (-0.5)
    grad_parts = []
    grad_keys = jnp.zeros((count, head), jnp.float32)
    grad_values = jnp.zeros((count, head), jnp.float32)
    for index in range(heads):
        cols = slice(index * head, (index + 1) * head)
        q_head = q_rows[:, cols]
        d_head = d_attn[:, cols]
        delta = jnp.sum(
            d_head.astype(jnp.float32) * attn_rows[:, cols].astype(jnp.float32),
            axis=1,
            keepdims=True,
        )
        d_prob = lax.dot_general(
            d_head, values, (((1,), (1,)), ((), ())), preferred_element_type=jnp.float32
        )
        d_score = (probs[index] * (d_prob - delta)).astype(jnp.bfloat16)
        grad_parts.append(jnp.dot(d_score, keys, preferred_element_type=jnp.float32) * scale)
        grad_keys = (
            grad_keys
            + lax.dot_general(
                d_score, q_head, (((0,), (0,)), ((), ())), preferred_element_type=jnp.float32
            )
            * scale
        )
        grad_values = grad_values + lax.dot_general(
            probs[index].astype(jnp.bfloat16),
            d_head,
            (((0,), (0,)), ((), ())),
            preferred_element_type=jnp.float32,
        )
    grad_q = jnp.concatenate(grad_parts, axis=1).astype(jnp.bfloat16)
    grad_kv = jnp.concatenate([grad_keys, grad_values], axis=1).astype(jnp.bfloat16)
    return (grad_q, grad_kv)


def on_device(queries, keys_values, seg_ids, in_resp, advantage, out_weight, upstream):
    attn_rows, probs = attend_forward(queries, keys_values, seg_ids)
    whole_weight = lax.all_gather(out_weight, "fsdp", axis=1, tiled=True)
    branch = jnp.dot(attn_rows, whole_weight, preferred_element_type=jnp.float32)
    branch_out = branch.astype(jnp.bfloat16)
    resp_total = lax.psum(jnp.sum(in_resp), ("dp", "fsdp"))
    all_tokens = queries.shape[0] * lax.axis_size("dp") * lax.axis_size("fsdp")
    factor = -(jnp.float32(all_tokens) / resp_total.astype(jnp.float32))
    coef = factor * in_resp.astype(jnp.float32) * (advantage.astype(jnp.float32) * 0.125)
    d_out = (coef[:, None] * upstream.astype(jnp.float32)).astype(jnp.bfloat16)
    d_attn = lax.dot_general(
        d_out, whole_weight, (((1,), (1,)), ((), ())), preferred_element_type=jnp.float32
    )
    d_attn = d_attn.astype(jnp.bfloat16)
    partial_value = lax.dot_general(
        attn_rows, d_out, (((0,), (0,)), ((), ())), preferred_element_type=jnp.float32
    )
    column_sums = lax.psum_scatter(
        partial_value.astype(jnp.bfloat16), "fsdp", scatter_dimension=1, tiled=True
    ).astype(jnp.float32)
    grad_weight = lax.psum_scatter(column_sums, "dp", scatter_dimension=0, tiled=True)
    grad_q, grad_kv = attend_backward(queries, keys_values, attn_rows, d_attn, probs)
    return (branch_out, grad_q, grad_kv, grad_weight)


def solution(mesh):
    in_specs = (
        P(("dp", "fsdp"), None),
        P(("dp", "fsdp"), None),
        P(("dp", "fsdp")),
        P(("dp", "fsdp")),
        P(("dp", "fsdp")),
        P(None, "fsdp"),
        P(("dp", "fsdp"), None),
    )
    out_specs = (
        P(("dp", "fsdp"), None),
        P(("dp", "fsdp"), None),
        P(("dp", "fsdp"), None),
        P("dp", "fsdp"),
    )
    nd, nf = mesh.shape["dp"], mesh.shape["fsdp"]

    def on_each(queries, keys_values, seg_ids, in_resp, advantage, out_weight, upstream):
        args = (queries, keys_values, seg_ids, in_resp, advantage, out_weight, upstream)
        depth, cols = out_weight.shape
        head = keys_values.shape[1] // 2
        heads = depth // head
        fits = (
            nd % 4 == 0 and nf % 2 == 0 and heads % 2 == 0 and depth % (16 * nd) == 0
            and cols % 128 == 0 and head % 128 == 0 and depth % (16 * W_CHUNKS) == 0
        )
        if fits:
            return fused(nd, nf, *args)
        return on_device(*args)

    return jax.shard_map(
        on_each, mesh=mesh, in_specs=in_specs, out_specs=out_specs, check_vma=False
    )
```

```python
import functools

import jax
import jax.numpy as jnp
from jax import lax
from jax.experimental import pallas as pl
from jax.experimental.pallas import tpu as pltpu
from jax.sharding import PartitionSpec as P

MESH = pl.DeviceIdType.MESH
neg_fill = -1e30
bf16 = jnp.bfloat16
f32 = jnp.float32
W_CHUNKS = 3


def dot(a, b, dims):
    return lax.dot_general(a, b, ((dims[0], dims[1]), ((), ())), preferred_element_type=f32)


def fused_kernel(
    sizes,
    q_hbm, kv_hbm, seg_hbm, resp_hbm, adv_hbm, w_hbm, up_hbm,
    bo, gq, gkv, gw,
    q, kv, seg, resp, adv, up,
    w_all, d_out, attn, prob, d_attn, bias, cnt,
    part, c_recv, x_send, x_recv, z_send, z_recv, y_send, y_recv,
    cnt_y, cnt_z,
    load_sem,
    ws_sem, wr_sem, cs_sem, cr_sem, xs_sem, xr_sem, zs_sem, zr_sem, ys_sem, yr_sem,
    ns_sem, nr_sem, nys_sem, nyr_sem, nzs_sem, nzr_sem,
):
    nd, nf, tok, heads, head, rows, cols = sizes
    nz, ny = nd // 2, nf // 2
    half_heads, half_blocks, half_z = heads // 2, nd // 2, nz // 2
    scale = head ** (-0.5)
    dp, fs = lax.axis_index("dp"), lax.axis_index("fsdp")
    c, y = lax.rem(fs, 2), lax.div(fs, 2)
    x, z = lax.rem(dp, 2), lax.div(dp, 2)
    sib_f = y * 2 + 1 - c
    sib = (dp, sib_f)
    x_peer = (z * 2 + 1 - x, fs)

    far = 1 - lax.div(z, half_z)
    halves = (far, 1 - far)

    def owners(n):
        base = halves[n] * half_z
        if n == 0:
            return [base + i for i in range(half_z)]
        return [base + lax.rem(z - base + 1 + i, half_z) for i in range(half_z)]

    def y_of(j):
        return lax.rem(y + j, ny)

    def z_of(k):
        return lax.rem(z + k, nz)

    def y_dev(j):
        return (dp, y_of(j) * 2 + c)

    def z_dev(k):
        return (z_of(k) * 2 + x, fs)

    def remote(src, dst, ss, rs, dev):
        return pltpu.make_async_remote_copy(
            src_ref=src, dst_ref=dst, send_sem=ss, recv_sem=rs, device_id=dev, device_id_type=MESH
        )

    sends = []

    def send(*args):
        copy = remote(*args)
        copy.start()
        sends.append(copy)

    loads = [
        pltpu.make_async_copy(a, b, load_sem.at[i])
        for i, (a, b) in enumerate(
            [(seg_hbm, seg), (resp_hbm, resp), (adv_hbm, adv), (q_hbm, q), (kv_hbm, kv),
             (up_hbm, up), (w_hbm, w_all.at[fs])]
        )
    ]
    for load in loads:
        load.start()

    loads[1].wait()
    count = jnp.sum(resp[...].astype(f32), axis=1, keepdims=True)
    cnt[0] = jnp.broadcast_to(count, cnt.shape[1:])

    barrier = pltpu.get_barrier_semaphore()
    peers = [sib, x_peer] + [y_dev(j) for j in range(1, ny)] + [z_dev(k) for k in range(1, nz)]
    for peer in peers:
        pl.semaphore_signal(barrier, inc=1, device_id=peer, device_id_type=MESH)
    pl.semaphore_wait(barrier, len(peers))
    for j in range(1, ny):
        send(cnt.at[0], cnt_y.at[y], nys_sem.at[j], nyr_sem.at[y], y_dev(j))

    depth = heads * head
    step = depth // W_CHUNKS

    def w_rows(i):
        return pl.ds(i * step, step)

    for i in range(W_CHUNKS):
        for j in range(1, ny):
            send(w_hbm.at[w_rows(i)], w_all.at[fs, w_rows(i)], ws_sem.at[j, i], wr_sem.at[fs, i], y_dev(j))
    for i in range(W_CHUNKS):
        send(w_hbm.at[w_rows(i)], w_all.at[fs, w_rows(i)], ws_sem.at[0, i], wr_sem.at[fs, i], sib)

    def w_wait(shard, i):
        ref = w_all.at[shard, w_rows(i)]
        remote(ref, ref, ws_sem.at[0, i], wr_sem.at[shard, i], sib).wait_recv()

    def w_forward(i):
        for j in range(1, ny):
            shard = y_of(j) * 2 + c
            w_wait(shard, i)
            send(w_all.at[shard, w_rows(i)], w_all.at[shard, w_rows(i)],
                 ws_sem.at[ny - 1 + j, i], wr_sem.at[shard, i], sib)

    for load in (loads[0], loads[2]):
        load.wait()
    coef_row = resp[...].astype(f32) * (adv[...].astype(f32) * 0.125)
    coef = jnp.transpose(jnp.broadcast_to(coef_row, (128, tok)))[:, :1]
    seg_k = jnp.broadcast_to(seg[...].astype(f32), (tok, tok))
    seg_q = jnp.transpose(seg_k)
    at_q = lax.broadcasted_iota(jnp.int32, (tok, tok), 0)
    at_k = lax.broadcasted_iota(jnp.int32, (tok, tok), 1)
    bias[...] = jnp.where((seg_q == seg_k) & (at_k <= at_q), 0.0, neg_fill)
    for load in loads[3:6]:
        load.wait()
    for s in range(nf):
        d_out[s] = (coef * up[:, s * cols:(s + 1) * cols].astype(f32)).astype(bf16)
    keys, values = kv[:, :head], kv[:, head:]

    def lanes(h):
        return pl.ds(pl.multiple_of(h * head, 128), head)

    def forward(h):
        cut = lanes(h)
        scores = dot(q[:, cut], keys, ((1,), (1,))) * scale + bias[...]
        top = jnp.max(scores, axis=1, keepdims=True)
        expo = jnp.exp(scores - top)
        p = (expo * (1.0 / jnp.sum(expo, axis=1, keepdims=True))).astype(bf16)
        prob[h] = p
        attn[:, cut] = dot(p, values, ((1,), (0,))).astype(bf16)

    def partial(n):
        width = half_heads * head
        left = attn[:, pl.ds(pl.multiple_of(halves[n] * width, 128), width)]
        first = halves[n] * half_blocks
        blocks = pl.ds(first, half_blocks)

        def shard(s):
            got = dot(left, d_out[s], ((0,), (0,))).astype(bf16)
            for b in range(half_blocks):
                part[s, first + b] = got[b * rows:(b + 1) * rows]

        for j in range(1, ny + 1):
            yy = y_of(j)
            shard(yy * 2 + 1 - c)
            send(part.at[yy * 2 + 1 - c, blocks], c_recv.at[yy, blocks],
                 cs_sem.at[n, yy], cr_sem.at[n, yy], sib)
        for j in range(1, ny + 1):
            shard(y_of(j) * 2 + c)

    def x_order(n):
        zs = owners(n)
        return [(zz, j, n == 0 or zz is not zs[-1]) for j in range(1, ny + 1) for zz in zs]

    def c_stage(n):
        blocks = pl.ds(halves[n] * half_blocks, half_blocks)
        waited = set()
        for zz, j, _ in x_order(n):
            yy = y_of(j)
            if j not in waited:
                waited.add(j)
                ref = c_recv.at[yy, blocks]
                remote(ref, ref, cs_sem.at[n, yy], cr_sem.at[n, yy], sib).wait_recv()
            block = zz * 2 + 1 - x
            both = part[yy * 2 + c, block].astype(f32) + c_recv[yy, block].astype(f32)
            x_send[zz, yy] = both.astype(bf16)
            send(x_send.at[zz, yy], x_recv.at[zz, yy], xs_sem.at[zz, yy], xr_sem.at[zz, yy], x_peer)

    def x_stage(zz, j, leaves):
        yy = y_of(j)
        ref = x_recv.at[zz, yy]
        remote(ref, ref, xs_sem.at[zz, yy], xr_sem.at[zz, yy], x_peer).wait_recv()
        block = zz * 2 + x
        total = part[yy * 2 + c, block].astype(f32) + c_recv[yy, block].astype(f32) + ref[...].astype(f32)
        z_send[zz, yy] = total.astype(bf16)
        if leaves:
            send(z_send.at[zz, yy], z_recv.at[z, yy], zs_sem.at[zz, yy], zr_sem.at[z, yy],
                 (zz * 2 + x, fs))

    def z_stage(j):
        yy = y_of(j)
        total = z_send[z, yy].astype(f32)
        for k in range(1, nz):
            src = z_of(k)
            ref = z_recv.at[src, yy]
            remote(ref, ref, zs_sem.at[src, yy], zr_sem.at[src, yy], z_dev(k)).wait_recv()
            total = total + ref[...].astype(f32)
        return total

    def use_weight(s, first=False):
        w = w_all[s]
        bo[:, pl.ds(pl.multiple_of(s * cols, 128), cols)] = dot(attn[...], w, ((1,), (0,))).astype(bf16)
        grad = dot(d_out[s], w, ((1,), (1,)))
        d_attn[...] = grad if first else d_attn[...] + grad

    def count_y():
        total = cnt[0]
        for j in range(1, ny):
            ref = cnt_y.at[y_of(j)]
            remote(ref, ref, nys_sem.at[j], nyr_sem.at[y_of(j)], y_dev(j)).wait_recv()
            total = total + ref[...]
        cnt[1] = total
        send(cnt.at[1], cnt.at[2], ns_sem.at[0], nr_sem.at[0], sib)

    def count_core():
        remote(cnt.at[2], cnt.at[2], ns_sem.at[0], nr_sem.at[0], sib).wait_recv()
        cnt[3] = cnt[1] + cnt[2]
        send(cnt.at[3], cnt.at[4], ns_sem.at[1], nr_sem.at[1], x_peer)

    def count_x():
        remote(cnt.at[4], cnt.at[4], ns_sem.at[1], nr_sem.at[1], x_peer).wait_recv()
        cnt[5] = cnt[3] + cnt[4]
        for k in range(1, nz):
            send(cnt.at[5], cnt_z.at[z], nzs_sem.at[k], nzr_sem.at[z], z_dev(k))

    def count_z():
        total = cnt[5]
        for k in range(1, nz):
            ref = cnt_z.at[z_of(k)]
            remote(ref, ref, nzs_sem.at[k], nzr_sem.at[z_of(k)], z_dev(k)).wait_recv()
            total = total + ref[...]
        return -(f32(tok * nd * nf) / total[:1, :1])

    for i in range(half_heads):
        forward(halves[0] * half_heads + i)
    count_y()
    partial(0)
    count_core()
    for i in range(half_heads):
        forward(halves[1] * half_heads + i)
    c_stage(0)
    partial(1)
    count_x()
    c_stage(1)
    loads[6].wait()
    use_weight(fs, first=True)
    w_forward(0)
    for i in range(W_CHUNKS):
        w_wait(sib_f, i)
    use_weight(sib_f)

    state = {}

    def weights_of(j):
        shard = y_of(j) * 2 + c
        use_weight(shard)

    def weights_other(j):
        shard = y_of(j) * 2 + 1 - c
        for i in range(W_CHUNKS):
            w_wait(shard, i)
        use_weight(shard)

    def backward(h):
        if h == 0:
            state["factor"] = count_z()
            state["gk"] = jnp.zeros((tok, head), f32)
            state["gv"] = jnp.zeros((tok, head), f32)
        factor = state["factor"]
        cut = slice(h * head, (h + 1) * head)
        d_full = d_attn[:, cut]
        d_head = d_full.astype(bf16)
        delta = jnp.sum(d_head.astype(f32) * attn[:, cut].astype(f32), axis=1, keepdims=True)
        p = prob[h]
        d_prob = dot(d_head, values, ((1,), (1,)))
        d_score = (p.astype(f32) * (d_prob - delta)).astype(bf16)
        gq[:, cut] = (dot(d_score, keys, ((1,), (0,))) * (scale * factor)).astype(bf16)
        state["gk"] = state["gk"] + dot(d_score, q[:, cut], ((0,), (0,)))
        state["gv"] = state["gv"] + dot(p, d_head, ((0,), (0,)))
        if h == heads - 1:
            gkv[:, :head] = (state["gk"] * (scale * factor)).astype(bf16)
            gkv[:, head:] = (state["gv"] * factor).astype(bf16)

    x_steps = [item for n in range(2) for item in x_order(n)]
    plan = [[] for _ in x_steps]

    def place(eighth, work):
        plan[eighth * len(x_steps) // 8].append(work)

    place(1, lambda: w_forward(1))
    for i in range(2, W_CHUNKS):
        place(3, functools.partial(w_forward, i))
    for j in range(1, ny):
        place(4, functools.partial(weights_of, j))
    for j in range(1, ny):
        place(5, functools.partial(weights_other, j))
    for h in range(heads):
        place(6 if h < half_heads else 6, functools.partial(backward, h))
    for n, x_step in enumerate(x_steps):
        x_stage(*x_step)
        passed = n + 1 - ny * half_z
        if passed > 0 and passed % half_z == 0 and passed < ny * half_z:
            j = passed // half_z
            y_send[j - 1] = z_stage(j).astype(bf16)
            send(y_send.at[j - 1], y_recv.at[y], ys_sem.at[j - 1], yr_sem.at[y], y_dev(j))

        for work in plan[n]:
            work()

    factor = state["factor"]
    total = z_stage(ny)
    for j in range(1, ny):
        src = y_of(j)
        ref = y_recv.at[src]
        remote(ref, ref, ys_sem.at[j - 1], yr_sem.at[src], y_dev(j)).wait_recv()
        total = total + ref[...].astype(f32)
    gw[...] = total * factor

    for copy in sends:
        copy.wait_send()


def copy_out(a, b, c, d, a_hbm, b_hbm, c_hbm, d_hbm, sem):
    pairs = [(a, a_hbm), (b, b_hbm), (c, c_hbm), (d, d_hbm)]
    copies = [pltpu.make_async_copy(*pair, sem.at[i]) for i, pair in enumerate(pairs)]
    for copy in copies:
        copy.start()
    for copy in copies:
        copy.wait()


def fused(nd, nf, queries, keys_values, seg_ids, in_resp, advantage, out_weight, upstream):
    tok, depth = queries.shape
    head = keys_values.shape[1] // 2
    heads = depth // head
    cols = out_weight.shape[1]
    rows = depth // nd
    nz, ny = nd // 2, nf // 2
    hbm_spec = pl.BlockSpec(memory_space=pltpu.HBM)
    any_spec = pl.BlockSpec(memory_space=pl.ANY)
    V, D = pltpu.VMEM, pltpu.SemaphoreType.DMA
    results = pl.pallas_call(
        functools.partial(fused_kernel, (nd, nf, tok, heads, head, rows, cols)),
        out_shape=(
            pltpu.VMEM((tok, nf * cols), bf16),
            pltpu.VMEM((tok, depth), bf16),
            pltpu.VMEM((tok, 2 * head), bf16),
            pltpu.VMEM((rows, cols), f32),
        ),
        in_specs=[hbm_spec] * 7,
        out_specs=(pl.BlockSpec(memory_space=pltpu.VMEM),) * 4,
        scratch_shapes=[
            V((tok, depth), bf16), V((tok, 2 * head), bf16),
            V((1, tok), jnp.int32), V((1, tok), jnp.int32), V((1, tok), jnp.int32),
            V((tok, nf * cols), bf16),
            V((nf, depth, cols), bf16), V((nf, tok, cols), bf16),
            V((tok, depth), bf16), V((heads, tok, tok), bf16), V((tok, depth), f32),
            V((tok, tok), f32), V((6, 8, 128), f32),
            V((nf, nd, rows, cols), bf16), V((ny, nd, rows, cols), bf16),
            V((nz, ny, rows, cols), bf16), V((nz, ny, rows, cols), bf16),
            V((nz, ny, rows, cols), bf16), V((nz, ny, rows, cols), bf16),
            V((ny, rows, cols), bf16), V((ny, rows, cols), bf16),
            V((ny, 8, 128), f32), V((nz, 8, 128), f32),
            D((7,)),
            D((nf, W_CHUNKS)), D((nf, W_CHUNKS)),
            D((2, ny)), D((2, ny)), D((nz, ny)), D((nz, ny)), D((nz, ny)), D((nz, ny)),
            D((ny,)), D((ny,)),
            D((2,)), D((2,)), D((ny,)), D((ny,)), D((nz,)), D((nz,)),
        ],
        compiler_params=pltpu.CompilerParams(
            collective_id=0, has_side_effects=True, vmem_limit_bytes=60 * 1024 * 1024
        ),
    )(
        *[pltpu.with_memory_space_constraint(a, pltpu.HBM) for a in (
            queries, keys_values, seg_ids.reshape(1, -1), in_resp.reshape(1, -1),
            advantage.reshape(1, -1), out_weight, upstream,
        )]
    )
    return pl.pallas_call(
        copy_out,
        out_shape=tuple(pltpu.HBM(r.shape, r.dtype) for r in results),
        in_specs=[pl.BlockSpec(memory_space=pltpu.VMEM)] * 4,
        out_specs=(any_spec,) * 4,
        scratch_shapes=[D((4,))],
        compiler_params=pltpu.CompilerParams(vmem_limit_bytes=4 * 1024 * 1024),
    )(*results)


def attend_forward(q_rows, kv_rows, seg_rows):
    count = q_rows.shape[0]
    head = kv_rows.shape[1] // 2
    heads = q_rows.shape[1] // head
    keys = kv_rows[:, :head]
    values = kv_rows[:, head:]
    place = jnp.arange(count, dtype=jnp.int32)
    allowed = (seg_rows[:, None] == seg_rows[None, :]) & (place[None, :] <= place[:, None])
    scale = head ** (-0.5)
    outputs = []
    probs = []
    for index in range(heads):
        q_head = q_rows[:, index * head : (index + 1) * head]
        scores = (
            lax.dot_general(
                q_head, keys, (((1,), (1,)), ((), ())), preferred_element_type=jnp.float32
            )
            * scale
        )
        scores = jnp.where(allowed, scores, neg_fill)
        top = jnp.max(scores, axis=1, keepdims=True)
        expo = jnp.exp(scores - top)
        prob = expo / jnp.sum(expo, axis=1, keepdims=True)
        outputs.append(
            jnp.dot(prob.astype(jnp.bfloat16), values, preferred_element_type=jnp.float32)
        )
        probs.append(prob)
    return (jnp.concatenate(outputs, axis=1).astype(jnp.bfloat16), probs)


def attend_backward(q_rows, kv_rows, attn_rows, d_attn, probs):
    count = q_rows.shape[0]
    head = kv_rows.shape[1] // 2
    heads = q_rows.shape[1] // head
    keys = kv_rows[:, :head]
    values = kv_rows[:, head:]
    scale = head ** (-0.5)
    grad_parts = []
    grad_keys = jnp.zeros((count, head), jnp.float32)
    grad_values = jnp.zeros((count, head), jnp.float32)
    for index in range(heads):
        cols = slice(index * head, (index + 1) * head)
        q_head = q_rows[:, cols]
        d_head = d_attn[:, cols]
        delta = jnp.sum(
            d_head.astype(jnp.float32) * attn_rows[:, cols].astype(jnp.float32),
            axis=1,
            keepdims=True,
        )
        d_prob = lax.dot_general(
            d_head, values, (((1,), (1,)), ((), ())), preferred_element_type=jnp.float32
        )
        d_score = (probs[index] * (d_prob - delta)).astype(jnp.bfloat16)
        grad_parts.append(jnp.dot(d_score, keys, preferred_element_type=jnp.float32) * scale)
        grad_keys = (
            grad_keys
            + lax.dot_general(
                d_score, q_head, (((0,), (0,)), ((), ())), preferred_element_type=jnp.float32
            )
            * scale
        )
        grad_values = grad_values + lax.dot_general(
            probs[index].astype(jnp.bfloat16),
            d_head,
            (((0,), (0,)), ((), ())),
            preferred_element_type=jnp.float32,
        )
    grad_q = jnp.concatenate(grad_parts, axis=1).astype(jnp.bfloat16)
    grad_kv = jnp.concatenate([grad_keys, grad_values], axis=1).astype(jnp.bfloat16)
    return (grad_q, grad_kv)


def on_device(queries, keys_values, seg_ids, in_resp, advantage, out_weight, upstream):
    attn_rows, probs = attend_forward(queries, keys_values, seg_ids)
    whole_weight = lax.all_gather(out_weight, "fsdp", axis=1, tiled=True)
    branch = jnp.dot(attn_rows, whole_weight, preferred_element_type=jnp.float32)
    branch_out = branch.astype(jnp.bfloat16)
    resp_total = lax.psum(jnp.sum(in_resp), ("dp", "fsdp"))
    all_tokens = queries.shape[0] * lax.axis_size("dp") * lax.axis_size("fsdp")
    factor = -(jnp.float32(all_tokens) / resp_total.astype(jnp.float32))
    coef = factor * in_resp.astype(jnp.float32) * (advantage.astype(jnp.float32) * 0.125)
    d_out = (coef[:, None] * upstream.astype(jnp.float32)).astype(jnp.bfloat16)
    d_attn = lax.dot_general(
        d_out, whole_weight, (((1,), (1,)), ((), ())), preferred_element_type=jnp.float32
    )
    d_attn = d_attn.astype(jnp.bfloat16)
    partial_value = lax.dot_general(
        attn_rows, d_out, (((0,), (0,)), ((), ())), preferred_element_type=jnp.float32
    )
    column_sums = lax.psum_scatter(
        partial_value.astype(jnp.bfloat16), "fsdp", scatter_dimension=1, tiled=True
    ).astype(jnp.float32)
    grad_weight = lax.psum_scatter(column_sums, "dp", scatter_dimension=0, tiled=True)
    grad_q, grad_kv = attend_backward(queries, keys_values, attn_rows, d_attn, probs)
    return (branch_out, grad_q, grad_kv, grad_weight)


def solution(mesh):
    in_specs = (
        P(("dp", "fsdp"), None),
        P(("dp", "fsdp"), None),
        P(("dp", "fsdp")),
        P(("dp", "fsdp")),
        P(("dp", "fsdp")),
        P(None, "fsdp"),
        P(("dp", "fsdp"), None),
    )
    out_specs = (
        P(("dp", "fsdp"), None),
        P(("dp", "fsdp"), None),
        P(("dp", "fsdp"), None),
        P("dp", "fsdp"),
    )
    nd, nf = mesh.shape["dp"], mesh.shape["fsdp"]

    def on_each(queries, keys_values, seg_ids, in_resp, advantage, out_weight, upstream):
        args = (queries, keys_values, seg_ids, in_resp, advantage, out_weight, upstream)
        depth, cols = out_weight.shape
        head = keys_values.shape[1] // 2
        heads = depth // head
        fits = (
            nd % 4 == 0 and nf % 2 == 0 and heads % 2 == 0 and depth % (16 * nd) == 0
            and cols % 128 == 0 and head % 128 == 0 and depth % (16 * W_CHUNKS) == 0
        )
        if fits:
            return fused(nd, nf, *args)
        return on_device(*args)

    return jax.shard_map(
        on_each, mesh=mesh, in_specs=in_specs, out_specs=out_specs, check_vma=False
    )
```
